16 devices in a mesh: dp: 4 (over z, y), tp: 4 (over x, core).
Axes of the slice: x: 2, y: 2, z: 2, core: 2. Of those that a mesh axis runs over, the one named last changes fastest.
Arguments:
- hidden: bfloat16 [48, 264, 1408], P('dp'), parts along dimension 0
- inter_feats: bfloat16 [48, 264, 5, 1408], P('dp'), parts along dimension 0
- proj_grad: bfloat16 [48, 257, 2560], P('dp'), parts along dimension 0
- w_query: bfloat16 [1408, 16, 88], P(None, 'tp')
- w_key: bfloat16 [1408, 16, 88], P(None, 'tp')
- w_value: bfloat16 [1408, 16, 88], P(None, 'tp')
- w_out: bfloat16 [16, 88, 1408], P('tp')
- ln_params: float32 [4, 1408], replicated
- gate_params: float32 [2], replicated
- w_fc1: bfloat16 [1408, 6144], P(None, 'tp')
- b_fc1: float32 [6144], P('tp')
- w_fc2: bfloat16 [6144, 1408], P('tp')
- b_fc2: float32 [1408], replicated
- w_proj: bfloat16 [8448, 2560], P('tp')
- b_proj: float32 [2560], replicated
Outputs:
- output 1: bfloat16 [48, 257, 2560], P(('dp', 'tp')), parts along dimension 0
- output 2: bfloat16 [48, 264, 1408], P('dp'), parts along dimension 0
- output 3: bfloat16 [48, 264, 5, 1408], P('dp'), parts along dimension 0
- output 4: float32 [5632, 16, 88], P('dp', 'tp'), parts along dimension 0
- output 5: float32 [5632, 16, 88], P('dp', 'tp'), parts along dimension 0
- output 6: float32 [5632, 16, 88], P('dp', 'tp'), parts along dimension 0
- output 7: float32 [64, 88, 1408], P(('dp', 'tp')), parts along dimension 0
- output 8: float32 [16, 1408], P('dp'), parts along dimension 0
- output 9: float32 [8], P('dp'), parts along dimension 0
- output 10: float32 [5632, 6144], P('dp', 'tp'), parts along dimension 0
- output 11: float32 [24576], P(('dp', 'tp')), parts along dimension 0
- output 12: float32 [24576, 1408], P(('dp', 'tp')), parts along dimension 0
- output 13: float32 [5632], P('dp'), parts along dimension 0
- output 14: float32 [33792, 2560], P(('dp', 'tp')), parts along dimension 0
- output 15: float32 [10240], P('dp'), parts along dimension 0
There are 4 independent parts. The reference program is written for one: setup_inputs(seed, part) draws one part's arguments, and reference() takes and returns one part's arrays. A program takes and returns all parts, laid end to end along the dimension named above; an argument that names none is the same for every part.
All inputs are finite; a program needn't handle non-finite values.
Results may differ from the reference program's by a relative error of at most 0.0195166.
Values are sent between devices in bfloat16 or wider.
A program may use at most 1 GiB of HBM per device.

```python
import jax
import jax.numpy as jnp
from jax import lax

D = 1408
HEADS = 16
FF = 6144
PROJ_DIM = 2560
NPATCH = 16
NINTER = 5
N_TILES = 12

REAL_TOK = NPATCH * NPATCH + 1
PAD_TOK = (REAL_TOK + 7) // 8 * 8
HEAD_DIM = D // HEADS
FEAT_DIM = (NINTER + 1) * D
LN_EPS = 1e-5


def setup_inputs(seed: int = 0, part: int = 0) -> dict:
    part_keys = jax.random.split(jax.random.fold_in(jax.random.key(seed), part), 4)
    weight_keys = jax.random.split(jax.random.key(seed + 1), 12)

    def normal_draw(slot_id, dims_in, spread):
        return jax.random.normal(weight_keys[slot_id], dims_in, jnp.float32) * spread

    row_scale = jnp.where(jnp.arange(PAD_TOK) < REAL_TOK, 1.0, 30.0)[None, :, None]
    tile_mean = jax.random.normal(part_keys[0], (N_TILES, 1, D), jnp.float32)
    tok_noise = jax.random.normal(part_keys[1], (N_TILES, PAD_TOK, D), jnp.float32)
    hidden = (tile_mean + tok_noise * row_scale).astype(jnp.bfloat16)
    inter_draw = jax.random.normal(part_keys[2], (N_TILES, PAD_TOK, NINTER, D), jnp.float32)
    inter_feats = (inter_draw * row_scale[..., None]).astype(jnp.bfloat16)
    proj_grad = jax.random.normal(part_keys[3], (N_TILES, REAL_TOK, PROJ_DIM), jnp.float32).astype(jnp.bfloat16)
    ln_base = jnp.array([1.0, 0.0, 1.0, 0.0], jnp.float32)[:, None]
    return {
        'hidden': hidden,
        'inter_feats': inter_feats,
        'proj_grad': proj_grad,
        'w_query': normal_draw(0, (D, HEADS, HEAD_DIM), D ** -0.5).astype(jnp.bfloat16),
        'w_key': normal_draw(1, (D, HEADS, HEAD_DIM), D ** -0.5).astype(jnp.bfloat16),
        'w_value': normal_draw(2, (D, HEADS, HEAD_DIM), D ** -0.5).astype(jnp.bfloat16),
        'w_out': normal_draw(3, (HEADS, HEAD_DIM, D), D ** -0.5).astype(jnp.bfloat16),
        'ln_params': ln_base + normal_draw(4, (4, D), 0.3),
        'gate_params': jax.random.uniform(weight_keys[5], (2,), jnp.float32, 0.6, 1.2),
        'w_fc1': normal_draw(6, (D, FF), D ** -0.5).astype(jnp.bfloat16),
        'b_fc1': normal_draw(7, (FF,), 0.5),
        'w_fc2': normal_draw(8, (FF, D), FF ** -0.5).astype(jnp.bfloat16),
        'b_fc2': normal_draw(9, (D,), 0.5),
        'w_proj': normal_draw(10, (FEAT_DIM, PROJ_DIM), FEAT_DIM ** -0.5).astype(jnp.bfloat16),
        'b_proj': normal_draw(11, (PROJ_DIM,), 0.5),
    }


def layer_norm(values, ln_gain, ln_bias):
    row_mean = jnp.mean(values, axis=-1, keepdims=True)
    centred = values - row_mean
    row_var = jnp.mean(centred * centred, axis=-1, keepdims=True)
    return centred * lax.rsqrt(row_var + LN_EPS) * ln_gain + ln_bias


def tile_forward(tile_x, tile_inter, w_query, w_key, w_value, w_out, ln_params, gate_params, w_fc1, b_fc1, w_fc2, b_fc2, w_proj, b_proj):
    x_wide = tile_x.astype(jnp.float32)
    normed = layer_norm(x_wide, ln_params[0], ln_params[1]).astype(jnp.bfloat16)
    q_act = jnp.dot(normed, w_query.reshape(D, D), preferred_element_type=jnp.float32).astype(jnp.bfloat16).reshape(PAD_TOK, HEADS, HEAD_DIM)
    k_act = jnp.dot(normed, w_key.reshape(D, D), preferred_element_type=jnp.float32).astype(jnp.bfloat16).reshape(PAD_TOK, HEADS, HEAD_DIM)
    v_act = jnp.dot(normed, w_value.reshape(D, D), preferred_element_type=jnp.float32).astype(jnp.bfloat16).reshape(PAD_TOK, HEADS, HEAD_DIM)
    scores = jnp.einsum('qhe,khe->hqk', q_act.astype(jnp.float32), k_act.astype(jnp.float32)) * HEAD_DIM ** -0.5
    key_ok = jnp.arange(PAD_TOK) < REAL_TOK
    scores = jnp.where(key_ok[None, None, :], scores, -1e30)
    attn_probs = jax.nn.softmax(scores, axis=-1).astype(jnp.bfloat16)
    context = jnp.einsum('hqk,khe->qhe', attn_probs.astype(jnp.float32), v_act.astype(jnp.float32)).astype(jnp.bfloat16).reshape(PAD_TOK, D)
    attn_out = jnp.dot(context, w_out.reshape(D, D), preferred_element_type=jnp.float32)
    x_one = (x_wide + jnp.tanh(gate_params[0]) * attn_out).astype(jnp.bfloat16)
    x_one_wide = x_one.astype(jnp.float32)
    normed_two = layer_norm(x_one_wide, ln_params[2], ln_params[3]).astype(jnp.bfloat16)
    pre_act = jnp.dot(normed_two, w_fc1, preferred_element_type=jnp.float32) + b_fc1
    mlp_act = jax.nn.gelu(pre_act, approximate=False).astype(jnp.bfloat16)
    mlp_out = jnp.dot(mlp_act, w_fc2, preferred_element_type=jnp.float32) + b_fc2
    x_two = (x_one_wide + jnp.tanh(gate_params[1]) * mlp_out).astype(jnp.bfloat16)
    features = jnp.concatenate([x_two, tile_inter.reshape(PAD_TOK, NINTER * D)], axis=-1)[:REAL_TOK]
    return (jnp.dot(features, w_proj, preferred_element_type=jnp.float32) + b_proj).astype(jnp.bfloat16)


def reference(hidden, inter_feats, proj_grad, w_query, w_key, w_value, w_out, ln_params, gate_params, w_fc1, b_fc1, w_fc2, b_fc2, w_proj, b_proj):
    weights = (w_query, w_key, w_value, w_out, ln_params, gate_params, w_fc1, b_fc1, w_fc2, b_fc2, w_proj, b_proj)

    def tile_step(grad_acc, tile_data):
        tile_x, tile_inter, tile_grad = tile_data
        tile_out, pull_back = jax.vjp(tile_forward, tile_x, tile_inter, w_query, w_key, w_value, w_out, ln_params, gate_params, w_fc1, b_fc1, w_fc2, b_fc2, w_proj, b_proj)
        grad_list = pull_back(tile_grad)
        new_acc = tuple(acc_item + grad_item.astype(jnp.float32) for acc_item, grad_item in zip(grad_acc, grad_list[2:]))
        return new_acc, (tile_out, grad_list[0], grad_list[1])

    zero_grads = tuple(jnp.zeros(weight.shape, jnp.float32) for weight in weights)
    grad_acc, tile_results = lax.scan(tile_step, zero_grads, (hidden, inter_feats, proj_grad))
    proj_out, grad_hidden, grad_inter = tile_results
    return (proj_out, grad_hidden, grad_inter, grad_acc[0], grad_acc[1], grad_acc[2], grad_acc[3], grad_acc[4], grad_acc[5], grad_acc[6], grad_acc[7], grad_acc[8], grad_acc[9], grad_acc[10], grad_acc[11])
```

```python
import jax
import jax.numpy as jnp
from jax import lax
from jax.sharding import PartitionSpec as P

LN_EPS = 1e-5
F32 = jnp.float32
BF16 = jnp.bfloat16
SIB = [(0, 1), (1, 0), (2, 3), (3, 2)]
ACROSS = [(0, 2), (2, 0), (1, 3), (3, 1)]


def layer_norm(values, ln_gain, ln_bias):
    row_mean = jnp.mean(values, axis=-1, keepdims=True)
    centred = values - row_mean
    row_var = jnp.mean(centred * centred, axis=-1, keepdims=True)
    return (centred * lax.rsqrt(row_var + LN_EPS) * ln_gain + ln_bias).astype(BF16)


def mm(eq_form, lhs_in, rhs_in):
    return jnp.einsum(eq_form, lhs_in, rhs_in, preferred_element_type=F32)


def attend(real_rows, q_act, k_act, v_act):
    tokens = q_act.shape[2]
    score_scale = q_act.shape[3] ** -0.5
    scores = mm('bhqe,bhke->bhqk', q_act, k_act) * score_scale
    key_ok = (jnp.arange(tokens) < real_rows)[None, None, None, :]
    attn_probs = jax.nn.softmax(jnp.where(key_ok, scores, -1e30), axis=-1).astype(BF16)
    return mm('bhqk,bhke->bhqe', attn_probs, v_act).astype(BF16)


def sib(value):
    return lax.ppermute(value, 'tp', SIB)


def across(value):
    return lax.ppermute(value, 'tp', ACROSS)


def partner_shard(shard):
    rows = shard.shape[0] // 4
    quarter = lax.dynamic_slice_in_dim(shard, lax.axis_index('dp') * rows, rows, axis=0)
    return lax.all_gather(across(quarter), 'dp', axis=0, tiled=True)


def reduce_own(near, far):
    n = near.shape[0] // 2
    from_sib_own = sib(near[n:])
    from_sib_far = sib(far[n:])
    chip_far = (far[:n].astype(F32) + from_sib_far.astype(F32)).astype(BF16)
    from_far = across(chip_far)
    return near[:n].astype(F32) + from_sib_own.astype(F32) + from_far.astype(F32)


def by_tp(tp, parts, builders):
    return lax.switch(tp, [lambda *p, b=b: b(*p) for b in builders], *parts)


def local_step(hidden, inter_feats, proj_grad, w_query, w_key, w_value, w_out, ln_params, gate_params, w_fc1, b_fc1, w_fc2, b_fc2, w_proj, b_proj):
    tiles, tokens, width = hidden.shape
    real_rows, proj_dim = proj_grad.shape[1:]
    ninter = inter_feats.shape[2]
    own_n = tiles // 4
    tp = lax.axis_index('tp')
    core = tp % 2
    first = tp * own_n
    inter_t = jnp.transpose(inter_feats, (0, 2, 1, 3))
    row_ok = (jnp.arange(tokens) < real_rows)[None, :, None]
    gate_attn = jnp.tanh(gate_params[0])
    gate_mlp = jnp.tanh(gate_params[1])

    def own(value):
        return lax.dynamic_slice_in_dim(value, first, own_n, axis=0)

    def group_of(value, other):
        return lax.dynamic_slice_in_dim(value, (tp ^ other) * own_n, own_n, axis=0)

    att_own = jnp.stack([jnp.transpose(w_query, (1, 2, 0)), jnp.transpose(w_key, (1, 2, 0)), jnp.transpose(w_value, (1, 2, 0)), w_out])
    heads, head_dim = att_own.shape[1:3]
    att_rows = att_own.reshape(4 * heads * head_dim, width)
    att_far = partner_shard(att_rows)
    att_sib = sib(att_rows)
    att_far_sib = sib(att_far)
    att_all = jnp.concatenate([v.reshape(4, heads, head_dim, width) for v in (att_rows, att_far, att_sib, att_far_sib)], axis=1)
    wq, wk, wv, wo = att_all[0], att_all[1], att_all[2], att_all[3]

    wp_far = partner_shard(w_proj)
    wp_sib = sib(w_proj)
    wp_far_sib = sib(wp_far)

    def order(a, b, c, d):
        return a[:width], jnp.concatenate([a[width:], b, c, d], axis=0)

    wp_first, wp_rest = by_tp(tp, (w_proj, wp_sib, wp_far, wp_far_sib), [
        lambda o, s, f, fs: order(o, s, f, fs),
        lambda o, s, f, fs: order(s, o, fs, f),
        lambda o, s, f, fs: order(f, fs, o, s),
        lambda o, s, f, fs: order(fs, f, s, o)])
    wp_rest = wp_rest.reshape(ninter, width, proj_dim)

    pg = jnp.pad(proj_grad, ((0, 0), (0, tokens - real_rows), (0, 0)))

    hid_own = own(hidden).astype(F32)
    normed, norm1_pull = jax.vjp(layer_norm, hid_own, ln_params[0], ln_params[1])
    q_act = mm('btd,hed->bhte', normed, wq).astype(BF16)
    k_act = mm('btd,hed->bhte', normed, wk).astype(BF16)
    v_act = mm('btd,hed->bhte', normed, wv).astype(BF16)
    context, attend_pull = jax.vjp(lambda q, k, v: attend(real_rows, q, k, v), q_act, k_act, v_act)
    attn_out = mm('bhte,hed->btd', context, wo)
    x_one = (hid_own + gate_attn * attn_out).astype(BF16)

    x_far = across(x_one)
    x_sib = sib(x_one)
    x_far_sib = sib(x_far)
    x_near2 = jnp.concatenate([x_one, x_sib], axis=0)
    x_far2 = jnp.concatenate([x_far, x_far_sib], axis=0)

    grad_x_two = mm('btp,cp->btc', pg, wp_first).astype(BF16)
    gx_own = own(grad_x_two)
    grad_mlp_low = (gate_mlp * grad_x_two.astype(F32)).astype(BF16)
    gm_near = jnp.concatenate([own(grad_mlp_low), group_of(grad_mlp_low, 1)], axis=0)
    gm_far = jnp.concatenate([group_of(grad_mlp_low, 2), group_of(grad_mlp_low, 3)], axis=0)

    def mlp_part(x_part, gm_part):
        grad_act = mm('btd,fd->btf', gm_part, w_fc2).astype(BF16)
        normed_two = layer_norm(x_part.astype(F32), ln_params[2], ln_params[3])
        pre_act = mm('btd,df->btf', normed_two, w_fc1) + b_fc1
        cdf = 0.5 * (1.0 + lax.erf(pre_act * (0.5 ** 0.5)))
        pdf = jnp.exp(-0.5 * pre_act * pre_act) * 0.3989422804014327
        mlp_act = (pre_act * cdf).astype(BF16)
        grad_pre = grad_act.astype(F32) * (cdf + pre_act * pdf)
        grad_b = jnp.sum(grad_pre, axis=(0, 1))
        grad_pre_low = grad_pre.astype(BF16)
        mlp_sum = mm('btf,fd->btd', mlp_act, w_fc2).astype(BF16)
        grad_n = mm('btf,df->btd', grad_pre_low, w_fc1).astype(BF16)
        return normed_two, mlp_act, grad_pre_low, grad_b, mlp_sum, grad_n

    n2_near, act_near, gp_near, gb_near, m_near, gn_near = mlp_part(x_near2, gm_near)
    n2_far, act_far, gp_far, gb_far, m_far, gn_far = mlp_part(x_far2, gm_far)
    grad_b_fc1 = gb_near + gb_far
    grad_normed_two = reduce_own(gn_near, gn_far).astype(BF16)
    mlp_out = reduce_own(m_near, m_far) + b_fc2
    grad_w_fc1 = mm('btd,btf->df', n2_near, gp_near) + mm('btd,btf->df', n2_far, gp_far)
    grad_w_fc2 = mm('btf,btd->fd', act_near, gm_near) + mm('btf,btd->fd', act_far, gm_far)

    x_one_wide = x_one.astype(F32)
    x_two = jnp.where(row_ok, (x_one_wide + gate_mlp * mlp_out).astype(BF16), 0)
    proj_own = mm('btc,cp->btp', x_two, wp_first) + mm('bntc,ncp->btp', own(inter_t), wp_rest)
    proj_out = (proj_own[:, :real_rows] + b_proj).astype(BF16)
    x_two_far = lax.ppermute(x_two, 'tp', [(2, 0), (3, 1)])
    x_two_sib = lax.ppermute(x_two, 'tp', [(1, 0)])
    x_two_far_sib = lax.ppermute(x_two_far, 'tp', [(1, 0)])
    half = w_proj.shape[0] - width
    feats = by_tp(tp, (inter_t, x_two, x_two_sib, x_two_far, x_two_far_sib), [
        lambda i, o, s, f, fs: jnp.concatenate([jnp.concatenate([o, s, f, fs], axis=0), i[:, 0, :, :half]], axis=2),
        lambda i, o, s, f, fs: jnp.concatenate([i[:, 0, :, half:], i[:, 1]], axis=2),
        lambda i, o, s, f, fs: jnp.concatenate([i[:, 2], i[:, 3, :, :half]], axis=2),
        lambda i, o, s, f, fs: jnp.concatenate([i[:, 3, :, half:], i[:, 4]], axis=2)])
    grad_w_proj = mm('btc,btp->cp', feats, pg)

    pg_half = lax.dynamic_slice_in_dim(pg, core * (tiles // 2), tiles // 2, axis=0)
    gi_half = mm('btp,ncp->bntc', pg_half, wp_rest).astype(BF16)
    gi_sib = sib(gi_half)
    grad_inter = lax.cond(core == 0, lambda a, b: jnp.concatenate([a, b], axis=0), lambda a, b: jnp.concatenate([b, a], axis=0), gi_half, gi_sib)
    grad_inter = jnp.transpose(grad_inter, (0, 2, 1, 3))

    _, norm2_pull = jax.vjp(layer_norm, x_one_wide, ln_params[2], ln_params[3])
    grad_x_ln_two, grad_gain_two, grad_bias_two = norm2_pull(grad_normed_two)
    gx_own_wide = gx_own.astype(F32)
    grad_x_one = (gx_own_wide + grad_x_ln_two).astype(BF16).astype(F32)
    grad_attn_low = (gate_attn * grad_x_one).astype(BF16)
    grad_context = mm('btd,hed->bhte', grad_attn_low, wo).astype(BF16)
    grad_q, grad_k, grad_v = attend_pull(grad_context)
    grad_normed = (mm('bhte,hed->btd', grad_q, wq) + mm('bhte,hed->btd', grad_k, wk) + mm('bhte,hed->btd', grad_v, wv)).astype(BF16)
    grad_x_ln, grad_gain, grad_bias = norm1_pull(grad_normed)
    gh_own = (grad_x_one + grad_x_ln).astype(BF16)
    gh_far = across(gh_own)
    gh_sib = sib(gh_own)
    gh_far_sib = sib(gh_far)
    grad_hidden = by_tp(tp, (gh_own, gh_sib, gh_far, gh_far_sib), [
        lambda o, s, f, fs: jnp.concatenate([o, s, f, fs], axis=0),
        lambda o, s, f, fs: jnp.concatenate([s, o, fs, f], axis=0),
        lambda o, s, f, fs: jnp.concatenate([f, fs, o, s], axis=0),
        lambda o, s, f, fs: jnp.concatenate([fs, f, s, o], axis=0)])

    dw = [mm('bhte,btd->hed', grad_q, normed), mm('bhte,btd->hed', grad_k, normed), mm('bhte,btd->hed', grad_v, normed), mm('bhte,btd->hed', context, grad_attn_low)]
    dw = jnp.stack([d.astype(BF16) for d in dw])
    dw_sib = sib(dw[:, 2 * heads:])
    dw_far = across((dw[:, heads:2 * heads].astype(F32) + dw_sib[:, heads:].astype(F32)).astype(BF16))
    dw_own = dw[:, :heads].astype(F32) + dw_sib[:, :heads].astype(F32) + dw_far.astype(F32)
    grad_w_query = jnp.transpose(dw_own[0], (2, 0, 1))
    grad_w_key = jnp.transpose(dw_own[1], (2, 0, 1))
    grad_w_value = jnp.transpose(dw_own[2], (2, 0, 1))
    grad_w_out = dw_own[3]

    grad_gate_mlp = jnp.sum(gx_own_wide * mlp_out) * (1.0 - gate_mlp * gate_mlp)
    grad_gate_attn = jnp.sum(grad_x_one * attn_out) * (1.0 - gate_attn * gate_attn)
    small = jnp.concatenate([
        grad_gain, grad_bias, grad_gain_two, grad_bias_two,
        jnp.sum(gate_mlp * gx_own_wide, axis=(0, 1)),
        jnp.sum(own(proj_grad), axis=(0, 1), dtype=F32),
        grad_gate_attn[None], grad_gate_mlp[None]])
    small = lax.psum(small, 'tp')
    grad_ln = small[:4 * width].reshape(4, width)
    grad_b_fc2 = small[4 * width:5 * width]
    grad_b_proj = small[5 * width:5 * width + proj_dim]
    grad_gates = small[5 * width + proj_dim:]
    return (proj_out, grad_hidden, grad_inter, grad_w_query, grad_w_key, grad_w_value, grad_w_out, grad_ln, grad_gates, grad_w_fc1, grad_b_fc1, grad_w_fc2, grad_b_fc2, grad_w_proj, grad_b_proj)


def solution(mesh):
    tiles_spec = P('dp', None, None)
    inter_spec = P('dp', None, None, None)
    head_cols = P(None, 'tp', None)
    in_specs = (tiles_spec, inter_spec, tiles_spec, head_cols, head_cols, head_cols, P('tp', None, None), P(None, None), P(None), P(None, 'tp'), P('tp'), P('tp', None), P(None), P('tp', None), P(None))
    grad_heads = P('dp', 'tp', None)
    out_specs = (P(('dp', 'tp'), None, None), tiles_spec, inter_spec, grad_heads, grad_heads, grad_heads, P(('dp', 'tp'), None, None), P('dp', None), P('dp'), P('dp', 'tp'), P(('dp', 'tp')), P(('dp', 'tp'), None), P('dp'), P(('dp', 'tp'), None), P('dp'))
    return jax.shard_map(local_step, mesh=mesh, in_specs=in_specs, out_specs=out_specs, check_vma=False)
```

```python
import jax
import jax.numpy as jnp
from jax import lax
from jax.experimental import pallas as pl
from jax.sharding import PartitionSpec as P


LN_EPS = 1e-5
F32 = jnp.float32
BF16 = jnp.bfloat16
SIB = [(0, 1), (1, 0), (2, 3), (3, 2)]
ACROSS = [(0, 2), (2, 0), (1, 3), (3, 1)]


def layer_norm(values, ln_gain, ln_bias):
    row_mean = jnp.mean(values, axis=-1, keepdims=True)
    centred = values - row_mean
    row_var = jnp.mean(centred * centred, axis=-1, keepdims=True)
    return (centred * lax.rsqrt(row_var + LN_EPS) * ln_gain + ln_bias).astype(BF16)


def mm(eq_form, lhs_in, rhs_in):
    return jnp.einsum(eq_form, lhs_in, rhs_in, preferred_element_type=F32)


def attend(real_rows, q_act, k_act, v_act):
    tokens = q_act.shape[2]
    score_scale = q_act.shape[3] ** -0.5
    scores = mm('bhqe,bhke->bhqk', q_act, k_act) * score_scale
    key_ok = (jnp.arange(tokens) < real_rows)[None, None, None, :]
    attn_probs = jax.nn.softmax(jnp.where(key_ok, scores, -1e30), axis=-1).astype(BF16)
    return mm('bhqk,bhke->bhqe', attn_probs, v_act).astype(BF16)


def sib(value):
    return lax.ppermute(value, 'tp', SIB)


def across(value):
    return lax.ppermute(value, 'tp', ACROSS)


def partner_shard(shard, start, count):
    rows = count // 4
    quarter = lax.dynamic_slice_in_dim(shard, start + lax.axis_index('dp') * rows, rows, axis=0)
    quarter = across(quarter)
    return lax.all_gather(quarter, 'dp', axis=0, tiled=True)


def reduce_own(near, far):
    n = near.shape[0] // 2
    from_sib_far = sib(far[n:])
    from_sib_own = sib(near[n:])
    chip_far = (far[:n].astype(F32) + from_sib_far.astype(F32)).astype(BF16)
    from_far = across(chip_far)
    return near[:n].astype(F32) + from_sib_own.astype(F32) + from_far.astype(F32)


def by_tp(tp, parts, builders):
    return lax.switch(tp, [lambda *p, b=b: b(*p) for b in builders], *parts)


def unfilled(shape, dtype):
    return pl.pallas_call(
        lambda out_ref: None,
        out_shape=jax.ShapeDtypeStruct(shape, dtype),
        out_specs=pl.BlockSpec(memory_space=pl.ANY),
        name='unfilled')()


def put_rows(buffer, piece, start):
    return lax.dynamic_update_slice_in_dim(buffer, piece, start, axis=0)


def whole_step(hidden, inter_feats, proj_grad, w_query, w_key, w_value, w_out, ln_params, gate_params, w_fc1, b_fc1, w_fc2, b_fc2, w_proj, b_proj):
    tiles, tokens, width = hidden.shape
    real_rows, proj_dim = proj_grad.shape[1:]
    ninter = inter_feats.shape[2]
    own_n = tiles // 4
    tp = lax.axis_index('tp')
    core = tp & 1
    first = tp * own_n
    inter_t = jnp.transpose(inter_feats, (0, 2, 1, 3))
    row_ok = (jnp.arange(tokens) < real_rows)[None, :, None]
    gate_attn = jnp.tanh(gate_params[0])
    gate_mlp = jnp.tanh(gate_params[1])

    def own(value):
        return lax.dynamic_slice_in_dim(value, first, own_n, axis=0)

    def group_of(value, other):
        return lax.dynamic_slice_in_dim(value, (tp ^ other) * own_n, own_n, axis=0)

    att_own = jnp.stack([jnp.transpose(w_query, (1, 2, 0)), jnp.transpose(w_key, (1, 2, 0)), jnp.transpose(w_value, (1, 2, 0)), w_out])
    heads, head_dim = att_own.shape[1:3]
    att_rows = att_own.reshape(4 * heads * head_dim, width)
    att_sib = sib(att_rows)
    att_far = partner_shard(att_rows, 0, att_rows.shape[0])
    att_far_sib = sib(att_far)

    def head_group(*shards):
        return jnp.concatenate([v.reshape(4, heads, head_dim, width) for v in shards], axis=1)

    shard_rows = w_proj.shape[0]
    wp_sib = sib(w_proj)
    wp_far_head = partner_shard(w_proj, 0, width)
    wp_far_tail = partner_shard(w_proj, width, shard_rows - width)
    wp_far_sib_head = sib(wp_far_head)
    wp_far_sib_tail = sib(wp_far_tail)
    wp_all = unfilled((4 * shard_rows, proj_dim), BF16)
    wp_all = put_rows(wp_all, w_proj, tp * shard_rows)
    wp_all = put_rows(wp_all, wp_sib, (tp ^ 1) * shard_rows)
    wp_all = put_rows(wp_all, wp_far_head, (tp ^ 2) * shard_rows)
    wp_all = put_rows(wp_all, wp_far_sib_head, (tp ^ 3) * shard_rows)
    wp_all = put_rows(wp_all, wp_far_tail, (tp ^ 2) * shard_rows + width)
    wp_all = put_rows(wp_all, wp_far_sib_tail, (tp ^ 3) * shard_rows + width)
    wp_planes = wp_all.reshape(ninter + 1, width, proj_dim)
    wp_first = by_tp(tp, (w_proj, wp_sib, wp_far_head, wp_far_sib_head), [
        lambda o, s, f, fs: o[:width],
        lambda o, s, f, fs: s[:width],
        lambda o, s, f, fs: f,
        lambda o, s, f, fs: fs])

    pg = jnp.pad(proj_grad, ((0, 0), (0, tokens - real_rows), (0, 0)))

    hid_own = own(hidden).astype(F32)
    normed, norm1_pull = jax.vjp(layer_norm, hid_own, ln_params[0], ln_params[1])

    def attention(weights):
        wq, wk, wv, wo = weights[0], weights[1], weights[2], weights[3]
        q_act = mm('btd,hed->bhte', normed, wq).astype(BF16)
        k_act = mm('btd,hed->bhte', normed, wk).astype(BF16)
        v_act = mm('btd,hed->bhte', normed, wv).astype(BF16)
        context, pull = jax.vjp(lambda q, k, v: attend(real_rows, q, k, v), q_act, k_act, v_act)
        return mm('bhte,hed->btd', context, wo), context, pull

    w_near = head_group(att_rows, att_sib)
    attn_near, context_near, pull_near = attention(w_near)
    w_far = head_group(att_far, att_far_sib)
    attn_far, context_far, pull_far = attention(w_far)
    attn_out = attn_near + attn_far
    x_one = (hid_own + gate_attn * attn_out).astype(BF16)

    x_far = across(x_one)
    x_sib = sib(x_one)
    x_far_sib = sib(x_far)
    x_near2 = jnp.concatenate([x_one, x_sib], axis=0)
    x_far2 = jnp.concatenate([x_far, x_far_sib], axis=0)

    grad_x_two = mm('btp,cp->btc', pg, wp_first).astype(BF16)
    grad_mlp_low = (gate_mlp * grad_x_two.astype(F32)).astype(BF16)
    gx_own = own(grad_x_two)
    gm_near = jnp.concatenate([own(grad_mlp_low), group_of(grad_mlp_low, 1)], axis=0)
    gm_far = jnp.concatenate([group_of(grad_mlp_low, 2), group_of(grad_mlp_low, 3)], axis=0)

    def mlp_part(x_part, gm_part):
        grad_act = mm('btd,fd->btf', gm_part, w_fc2).astype(BF16)
        normed_two = layer_norm(x_part.astype(F32), ln_params[2], ln_params[3])
        pre_act = mm('btd,df->btf', normed_two, w_fc1) + b_fc1
        cdf = 0.5 * (1.0 + lax.erf(pre_act * (0.5 ** 0.5)))
        pdf = jnp.exp(-0.5 * pre_act * pre_act) * 0.3989422804014327
        mlp_act = (pre_act * cdf).astype(BF16)
        grad_pre = grad_act.astype(F32) * (cdf + pre_act * pdf)
        grad_b = jnp.sum(grad_pre, axis=(0, 1))
        grad_pre_low = grad_pre.astype(BF16)
        grad_n = mm('btf,df->btd', grad_pre_low, w_fc1).astype(BF16)
        mlp_sum = mm('btf,fd->btd', mlp_act, w_fc2).astype(BF16)
        return normed_two, mlp_act, grad_pre_low, grad_b, mlp_sum, grad_n

    n2_near, act_near, gp_near, gb_near, m_near, gn_near = mlp_part(x_near2, gm_near)
    n2_far, act_far, gp_far, gb_far, m_far, gn_far = mlp_part(x_far2, gm_far)
    grad_b_fc1 = gb_near + gb_far
    grad_normed_two = reduce_own(gn_near, gn_far).astype(BF16)
    mlp_out = reduce_own(m_near, m_far) + b_fc2
    grad_w_fc1 = mm('btd,btf->df', n2_near, gp_near) + mm('btd,btf->df', n2_far, gp_far)
    grad_w_fc2 = mm('btf,btd->fd', act_near, gm_near) + mm('btf,btd->fd', act_far, gm_far)

    x_one_wide = x_one.astype(F32)
    x_two = jnp.where(row_ok, (x_one_wide + gate_mlp * mlp_out).astype(BF16), 0)
    feats_own = jnp.concatenate([x_two[:, None], own(inter_t)], axis=1)
    proj_own = mm('bntc,ncp->btp', feats_own, wp_planes)
    proj_out = (proj_own[:, :real_rows] + b_proj).astype(BF16)
    x_two_far = lax.ppermute(x_two, 'tp', [(2, 0), (3, 1)])
    x_two_sib = lax.ppermute(x_two, 'tp', [(1, 0)])
    x_two_far_sib = lax.ppermute(x_two_far, 'tp', [(1, 0)])
    half = shard_rows - width
    feats = by_tp(tp, (inter_t, x_two, x_two_sib, x_two_far, x_two_far_sib), [
        lambda i, o, s, f, fs: jnp.concatenate([jnp.concatenate([o, s, f, fs], axis=0), i[:, 0, :, :half]], axis=2),
        lambda i, o, s, f, fs: jnp.concatenate([i[:, 0, :, half:], i[:, 1]], axis=2),
        lambda i, o, s, f, fs: jnp.concatenate([i[:, 2], i[:, 3, :, :half]], axis=2),
        lambda i, o, s, f, fs: jnp.concatenate([i[:, 3, :, half:], i[:, 4]], axis=2)])
    grad_w_proj = mm('btc,btp->cp', feats, pg)

    half_tiles = tiles // 2
    grad_inter = unfilled((tiles, ninter, tokens, width), BF16)
    gi_sib = []
    for n in range(ninter):
        pg_half = lax.dynamic_slice_in_dim(pg, core * half_tiles, half_tiles, axis=0)
        gi_half = mm('btp,cp->btc', pg_half, wp_planes[n + 1]).astype(BF16)
        grad_inter = lax.dynamic_update_slice(grad_inter, gi_half[:, None], (core * half_tiles, n, 0, 0))
        gi_sib.append(sib(gi_half))
    for n in range(ninter):
        grad_inter = lax.dynamic_update_slice(grad_inter, gi_sib[n][:, None], ((1 - core) * half_tiles, n, 0, 0))
    grad_inter = jnp.transpose(grad_inter, (0, 2, 1, 3))

    _, norm2_pull = jax.vjp(layer_norm, x_one_wide, ln_params[2], ln_params[3])
    grad_x_ln_two, grad_gain_two, grad_bias_two = norm2_pull(grad_normed_two)
    gx_own_wide = gx_own.astype(F32)
    grad_x_one = (gx_own_wide + grad_x_ln_two).astype(BF16).astype(F32)
    grad_attn_low = (gate_attn * grad_x_one).astype(BF16)

    def attention_back(weights, pull):
        grad_context = mm('btd,hed->bhte', grad_attn_low, weights[3]).astype(BF16)
        grad_q, grad_k, grad_v = pull(grad_context)
        partial = mm('bhte,hed->btd', grad_q, weights[0]) + mm('bhte,hed->btd', grad_k, weights[1]) + mm('bhte,hed->btd', grad_v, weights[2])
        return grad_q, grad_k, grad_v, partial

    def attention_dw(grad_q, grad_k, grad_v, context):
        parts = [mm('bhte,btd->hed', grad_q, normed), mm('bhte,btd->hed', grad_k, normed), mm('bhte,btd->hed', grad_v, normed), mm('bhte,btd->hed', context, grad_attn_low)]
        return jnp.stack([d.astype(BF16) for d in parts])

    gq_far, gk_far, gv_far, gnorm_far = attention_back(w_far, pull_far)
    dw_far2 = attention_dw(gq_far, gk_far, gv_far, context_far)
    dw_far_from_sib = sib(dw_far2[:, heads:])
    dw_from_far = across((dw_far2[:, :heads].astype(F32) + dw_far_from_sib.astype(F32)).astype(BF16))
    gq_near, gk_near, gv_near, gnorm_near = attention_back(w_near, pull_near)
    grad_normed = (gnorm_near + gnorm_far).astype(BF16)
    grad_x_ln, grad_gain, grad_bias = norm1_pull(grad_normed)
    gh_own = (grad_x_one + grad_x_ln).astype(BF16)
    gh_far = across(gh_own)
    gh_sib = sib(gh_own)
    gh_far_sib = sib(gh_far)
    dw_near2 = attention_dw(gq_near, gk_near, gv_near, context_near)
    dw_near_from_sib = sib(dw_near2[:, heads:])
    grad_hidden = by_tp(tp, (gh_own, gh_sib, gh_far, gh_far_sib), [
        lambda o, s, f, fs: jnp.concatenate([o, s, f, fs], axis=0),
        lambda o, s, f, fs: jnp.concatenate([s, o, fs, f], axis=0),
        lambda o, s, f, fs: jnp.concatenate([f, fs, o, s], axis=0),
        lambda o, s, f, fs: jnp.concatenate([fs, f, s, o], axis=0)])
    dw_own = dw_near2[:, :heads].astype(F32) + dw_near_from_sib.astype(F32) + dw_from_far.astype(F32)
    grad_w_query = jnp.transpose(dw_own[0], (2, 0, 1))
    grad_w_key = jnp.transpose(dw_own[1], (2, 0, 1))
    grad_w_value = jnp.transpose(dw_own[2], (2, 0, 1))
    grad_w_out = dw_own[3]

    mlp_out_late, _ = lax.optimization_barrier((mlp_out, grad_normed))
    grad_gate_mlp = jnp.sum(gx_own_wide * mlp_out_late) * (1.0 - gate_mlp * gate_mlp)
    grad_gate_attn = jnp.sum(grad_x_one * attn_out) * (1.0 - gate_attn * gate_attn)
    small = jnp.concatenate([
        grad_gain, grad_bias, grad_gain_two, grad_bias_two,
        jnp.sum(gate_mlp * gx_own_wide, axis=(0, 1)),
        jnp.sum(own(proj_grad), axis=(0, 1), dtype=F32),
        grad_gate_attn[None], grad_gate_mlp[None]])
    small = small + sib(small)
    small = small + across(small)
    grad_ln = small[:4 * width].reshape(4, width)
    grad_b_fc2 = small[4 * width:5 * width]
    grad_b_proj = small[5 * width:5 * width + proj_dim]
    grad_gates = small[5 * width + proj_dim:]
    return (proj_out, grad_hidden, grad_inter, grad_w_query, grad_w_key, grad_w_value, grad_w_out, grad_ln, grad_gates, grad_w_fc1, grad_b_fc1, grad_w_fc2, grad_b_fc2, grad_w_proj, grad_b_proj)


def solution(mesh):
    tiles_spec = P('dp', None, None)
    inter_spec = P('dp', None, None, None)
    head_cols = P(None, 'tp', None)
    in_specs = (tiles_spec, inter_spec, tiles_spec, head_cols, head_cols, head_cols, P('tp', None, None), P(None, None), P(None), P(None, 'tp'), P('tp'), P('tp', None), P(None), P('tp', None), P(None))
    grad_heads = P('dp', 'tp', None)
    out_specs = (P(('dp', 'tp'), None, None), tiles_spec, inter_spec, grad_heads, grad_heads, grad_heads, P(('dp', 'tp'), None, None), P('dp', None), P('dp'), P('dp', 'tp'), P(('dp', 'tp')), P(('dp', 'tp'), None), P('dp'), P(('dp', 'tp'), None), P('dp'))
    return jax.shard_map(whole_step, mesh=mesh, in_specs=in_specs, out_specs=out_specs, check_vma=False)
```

```python
import functools

import jax
import jax.numpy as jnp
from jax import lax
from jax.experimental import pallas as pl
from jax.experimental.pallas import tpu as pltpu
from jax.sharding import PartitionSpec as P


LN_EPS = 1e-5
TO_F = 'btd,fd->btf'
FROM_F = 'btf,fd->btd'
WGRAD = 'btf,btd->fd'
F32 = jnp.float32
BF16 = jnp.bfloat16
SIB = [(0, 1), (1, 0), (2, 3), (3, 2)]
ACROSS = [(0, 2), (2, 0), (1, 3), (3, 1)]


def layer_norm(values, ln_gain, ln_bias):
    row_mean = jnp.mean(values, axis=-1, keepdims=True)
    centred = values - row_mean
    row_var = jnp.mean(centred * centred, axis=-1, keepdims=True)
    return (centred * lax.rsqrt(row_var + LN_EPS) * ln_gain + ln_bias).astype(BF16)


def mm(eq_form, lhs_in, rhs_in):
    return jnp.einsum(eq_form, lhs_in, rhs_in, preferred_element_type=F32)


LANES = 128


def probs_t(q_block, k_block, real_rows, scale):
    scores = lax.dot_general(k_block, q_block, (((1,), (1,)), ((), ())), preferred_element_type=F32) * scale
    key = lax.broadcasted_iota(jnp.int32, scores.shape, 0)
    scores = jnp.where(key < real_rows, scores, -1e30)
    top = jnp.max(scores, axis=0, keepdims=True)
    expd = jnp.exp(scores - top)
    return expd * (1.0 / jnp.sum(expd, axis=0, keepdims=True))


def attend_kernel(real_rows, scale, count, q_ref, k_ref, v_ref, out_ref):
    for h in range(count):
        cols = pl.ds(h * LANES, LANES)
        probs = probs_t(q_ref[0, :, cols], k_ref[0, :, cols], real_rows, scale).astype(BF16)
        out = lax.dot_general(probs, v_ref[0, :, cols], (((0,), (0,)), ((), ())), preferred_element_type=F32)
        out_ref[0, :, cols] = out.astype(BF16)


def attend_back_kernel(real_rows, scale, count, q_ref, k_ref, v_ref, g_ref, dq_ref, dk_ref, dv_ref):
    for h in range(count):
        cols = pl.ds(h * LANES, LANES)
        q_block, k_block, v_block, g_block = q_ref[0, :, cols], k_ref[0, :, cols], v_ref[0, :, cols], g_ref[0, :, cols]
        probs = probs_t(q_block, k_block, real_rows, scale)
        dv_ref[0, :, cols] = jnp.dot(probs.astype(BF16), g_block, preferred_element_type=F32).astype(BF16)
        dprobs = lax.dot_general(v_block, g_block, (((1,), (1,)), ((), ())), preferred_element_type=F32).astype(BF16).astype(F32)
        dscores = probs * (dprobs - jnp.sum(probs * dprobs, axis=0, keepdims=True))
        dscores = (dscores * scale).astype(BF16)
        dk_ref[0, :, cols] = jnp.dot(dscores, q_block, preferred_element_type=F32).astype(BF16)
        dq = lax.dot_general(dscores, k_block, (((0,), (0,)), ((), ())), preferred_element_type=F32)
        dq_ref[0, :, cols] = dq.astype(BF16)


HEADS_PER_STEP = 4


def attend(q_act, k_act, v_act, real_rows, scale):
    tiles, tokens, cols = q_act.shape
    step = HEADS_PER_STEP * LANES
    spec = pl.BlockSpec((1, tokens, step), lambda t, h: (t, 0, h))
    flops = 4 * tiles * tokens * tokens * cols
    return pl.pallas_call(
        functools.partial(attend_kernel, real_rows, scale, HEADS_PER_STEP),
        out_shape=jax.ShapeDtypeStruct(q_act.shape, BF16),
        grid=(tiles, cols // step),
        in_specs=[spec] * 3,
        out_specs=spec,
        cost_estimate=pl.CostEstimate(flops=4 * flops, bytes_accessed=8 * tiles * tokens * cols, transcendentals=0),
        compiler_params=pltpu.CompilerParams(dimension_semantics=('arbitrary', 'arbitrary')))(q_act, k_act, v_act)


def attend_back(qkv, grad, real_rows, scale):
    tiles, tokens, cols = grad.shape
    step = HEADS_PER_STEP * LANES
    spec = pl.BlockSpec((1, tokens, step), lambda t, h: (t, 0, h))
    shape = jax.ShapeDtypeStruct(grad.shape, BF16)
    flops = 10 * tiles * tokens * tokens * cols
    return pl.pallas_call(
        functools.partial(attend_back_kernel, real_rows, scale, HEADS_PER_STEP),
        out_shape=(shape, shape, shape),
        grid=(tiles, cols // step),
        in_specs=[spec] * 4,
        out_specs=(spec, spec, spec),
        cost_estimate=pl.CostEstimate(flops=4 * flops, bytes_accessed=14 * tiles * tokens * cols, transcendentals=0),
        compiler_params=pltpu.CompilerParams(dimension_semantics=('arbitrary', 'arbitrary')))(*qkv, grad)


def sib(value):
    return lax.ppermute(value, 'tp', SIB)


def across(value):
    return lax.ppermute(value, 'tp', ACROSS)


def gather_piece(quarter):
    quarter = across(quarter)
    return lax.all_gather(quarter, 'dp', axis=0, tiled=True)


def partner_shard(shard, start, count):
    rows = count // 4
    quarter = lax.dynamic_slice_in_dim(shard, start + lax.axis_index('dp') * rows, rows, axis=0)
    return gather_piece(quarter)


def reduce_own(near, far):
    n = near.shape[0] // 2
    from_sib_far = sib(far[n:])
    from_sib_own = sib(near[n:])
    chip_far = (far[:n].astype(F32) + from_sib_far.astype(F32)).astype(BF16)
    from_far = across(chip_far)
    return near[:n].astype(F32) + from_sib_own.astype(F32) + from_far.astype(F32)


def by_tp(tp, parts, builders):
    return lax.switch(tp, [lambda *p, b=b: b(*p) for b in builders], *parts)


def unfilled(shape, dtype):
    return pl.pallas_call(
        lambda out_ref: None,
        out_shape=jax.ShapeDtypeStruct(shape, dtype),
        out_specs=pl.BlockSpec(memory_space=pl.ANY),
        name='unfilled')()


def put_rows(buffer, piece, start):
    return lax.dynamic_update_slice_in_dim(buffer, piece, start, axis=0)


def whole_step(hidden, inter_feats, proj_grad, w_query, w_key, w_value, w_out, ln_params, gate_params, w_fc1, b_fc1, w_fc2, b_fc2, w_proj, b_proj):
    tiles, tokens, width = hidden.shape
    real_rows, proj_dim = proj_grad.shape[1:]
    ninter = inter_feats.shape[2]
    own_n = tiles // 4
    tp = lax.axis_index('tp')
    core = tp & 1
    first = tp * own_n
    inter_t = jnp.transpose(inter_feats, (0, 2, 1, 3))
    row_ok = (jnp.arange(tokens) < real_rows)[None, :, None]
    gate_attn = jnp.tanh(gate_params[0])
    gate_mlp = jnp.tanh(gate_params[1])

    def own(value):
        return lax.dynamic_slice_in_dim(value, first, own_n, axis=0)

    def group_of(value, other):
        return lax.dynamic_slice_in_dim(value, (tp ^ other) * own_n, own_n, axis=0)

    att_own = jnp.stack([jnp.transpose(w_query, (1, 2, 0)), jnp.transpose(w_key, (1, 2, 0)), jnp.transpose(w_value, (1, 2, 0)), w_out])
    heads, head_dim = att_own.shape[1:3]
    att_rows = att_own.reshape(4 * heads * head_dim, width)
    att_sib = sib(att_rows)
    att_far = partner_shard(att_rows, 0, att_rows.shape[0])
    att_far_sib = sib(att_far)

    score_scale = head_dim ** -0.5

    def head_group(*shards):
        group = jnp.concatenate([v.reshape(4, heads, head_dim, width) for v in shards], axis=1)
        group = jnp.pad(group, ((0, 0), (0, 0), (0, LANES - head_dim), (0, 0)))
        return group.reshape(4, -1, width)

    shard_rows = w_proj.shape[0]
    half = shard_rows - width
    wp_sib = sib(w_proj)

    def far_head(own_core):
        quarter = half // 4
        start = core * half + lax.axis_index('dp') * quarter
        piece = jnp.where(core == own_core, lax.dynamic_slice_in_dim(w_proj, start, quarter), lax.dynamic_slice_in_dim(wp_sib, start, quarter))
        mine = gather_piece(piece)
        return mine, sib(mine)

    even, even_sib = far_head(0)
    odd, odd_sib = far_head(1)
    tail = partner_shard(w_proj, width, half)
    tail_sib = sib(tail)
    far_even = 2 * (1 - tp // 2) * shard_rows
    far_odd = far_even + shard_rows
    wp_all = unfilled((4 * shard_rows, proj_dim), BF16)
    wp_all = put_rows(wp_all, w_proj, tp * shard_rows)
    wp_all = put_rows(wp_all, wp_sib, (tp ^ 1) * shard_rows)
    for start, mine, other in ((far_even, even, even_sib), (far_odd, odd, odd_sib)):
        wp_all = put_rows(wp_all, mine, start + core * half)
        wp_all = put_rows(wp_all, other, start + (1 - core) * half)
    wp_all = put_rows(wp_all, tail, (tp ^ 2) * shard_rows + width)
    wp_all = put_rows(wp_all, tail_sib, (tp ^ 3) * shard_rows + width)
    wp_planes = wp_all.reshape(ninter + 1, width, proj_dim)
    wp_first = by_tp(tp, (w_proj, wp_sib, even, even_sib), [
        lambda o, s, e, es: o[:width],
        lambda o, s, e, es: s[:width],
        lambda o, s, e, es: jnp.concatenate([e, es], axis=0),
        lambda o, s, e, es: jnp.concatenate([es, e], axis=0)])

    pg = jnp.pad(proj_grad, ((0, 0), (0, tokens - real_rows), (0, 0)))

    hid_own = own(hidden).astype(F32)
    normed, norm1_pull = jax.vjp(layer_norm, hid_own, ln_params[0], ln_params[1])

    def attention(weights):
        qkv = [mm(TO_F, normed, weights[j]).astype(BF16) for j in range(3)]
        context = attend(*qkv, real_rows, score_scale)
        return mm(FROM_F, context, weights[3]), context, qkv

    w_near = head_group(att_rows, att_sib)
    attn_near, context_near, qkv_near = attention(w_near)
    w_far = head_group(att_far, att_far_sib)
    attn_far, context_far, qkv_far = attention(w_far)
    attn_out = attn_near + attn_far
    x_one = (hid_own + gate_attn * attn_out).astype(BF16)

    x_far = across(x_one)
    x_sib = sib(x_one)
    x_far_sib = sib(x_far)
    x_all = jnp.concatenate([x_one, x_sib, x_far, x_far_sib], axis=0)

    grad_x_two = mm(TO_F, pg, wp_first).astype(BF16)
    grad_mlp_low = (gate_mlp * grad_x_two.astype(F32)).astype(BF16)
    gx_own = own(grad_x_two)
    gm_all = jnp.concatenate([own(grad_mlp_low), group_of(grad_mlp_low, 1), group_of(grad_mlp_low, 2), group_of(grad_mlp_low, 3)], axis=0)

    grad_act = mm(TO_F, gm_all, w_fc2).astype(BF16)
    normed_two = layer_norm(x_all.astype(F32), ln_params[2], ln_params[3])
    pre_act = mm('btd,df->btf', normed_two, w_fc1) + b_fc1
    cdf = 0.5 * (1.0 + lax.erf(pre_act * (0.5 ** 0.5)))
    pdf = jnp.exp(-0.5 * pre_act * pre_act) * 0.3989422804014327
    mlp_act = (pre_act * cdf).astype(BF16)
    grad_pre = grad_act.astype(F32) * (cdf + pre_act * pdf)
    grad_b_fc1 = jnp.sum(grad_pre, axis=(0, 1))
    grad_pre_low = grad_pre.astype(BF16)
    pair = 2 * own_n
    gn_far = mm(TO_F, grad_pre_low[pair:], w_fc1).astype(BF16)
    gn_near = mm(TO_F, grad_pre_low[:pair], w_fc1).astype(BF16)
    mlp_sum = mm(FROM_F, mlp_act, w_fc2).astype(BF16)
    grad_normed_two = reduce_own(gn_near, gn_far).astype(BF16)
    mlp_out = reduce_own(mlp_sum[:pair], mlp_sum[pair:]) + b_fc2
    grad_w_fc1 = mm(WGRAD, normed_two, grad_pre_low)
    grad_w_fc2 = mm(WGRAD, mlp_act, gm_all)

    x_one_wide = x_one.astype(F32)
    x_two = jnp.where(row_ok, (x_one_wide + gate_mlp * mlp_out).astype(BF16), 0)
    feats_own = jnp.concatenate([x_two[:, None], own(inter_t)], axis=1)
    proj_own = mm('bntc,ncp->btp', feats_own, wp_planes)
    proj_out = (proj_own[:, :real_rows] + b_proj).astype(BF16)
    x_two_far = lax.ppermute(x_two, 'tp', [(2, 0), (3, 1)])
    x_two_sib = lax.ppermute(x_two, 'tp', [(1, 0)])
    x_two_far_sib = lax.ppermute(x_two_far, 'tp', [(1, 0)])
    part = by_tp(tp, (inter_t,), [
        lambda i: i[:, 0, :, :half],
        lambda i: i[:, 0, :, half:],
        lambda i: i[:, 3, :, :half],
        lambda i: i[:, 3, :, half:]])
    grad_w_proj = unfilled((shard_rows, proj_dim), F32)
    grad_w_proj = put_rows(grad_w_proj, mm(WGRAD, part, pg), (1 - core) * width)
    plane = by_tp(tp, (inter_t, x_two, x_two_sib, x_two_far, x_two_far_sib), [
        lambda i, o, s, f, fs: jnp.concatenate([o, s, f, fs], axis=0),
        lambda i, o, s, f, fs: i[:, 1],
        lambda i, o, s, f, fs: i[:, 2],
        lambda i, o, s, f, fs: i[:, 4]])
    grad_w_proj = put_rows(grad_w_proj, mm(WGRAD, plane, pg), core * half)

    half_tiles = tiles // 2
    grad_inter = unfilled((tiles, ninter, tokens, width), BF16)
    gi_sib = []
    for n in range(ninter):
        pg_half = lax.dynamic_slice_in_dim(pg, core * half_tiles, half_tiles, axis=0)
        gi_half = mm(TO_F, pg_half, wp_planes[n + 1]).astype(BF16)
        grad_inter = lax.dynamic_update_slice(grad_inter, gi_half[:, None], (core * half_tiles, n, 0, 0))
        gi_sib.append(sib(gi_half))
    for n in range(ninter):
        grad_inter = lax.dynamic_update_slice(grad_inter, gi_sib[n][:, None], ((1 - core) * half_tiles, n, 0, 0))
    grad_inter = jnp.transpose(grad_inter, (0, 2, 1, 3))

    _, norm2_pull = jax.vjp(layer_norm, x_one_wide, ln_params[2], ln_params[3])
    grad_x_ln_two, grad_gain_two, grad_bias_two = norm2_pull(grad_normed_two)
    gx_own_wide = gx_own.astype(F32)
    grad_x_one = (gx_own_wide + grad_x_ln_two).astype(BF16).astype(F32)
    grad_attn_low = (gate_attn * grad_x_one).astype(BF16)

    def attention_back(weights, qkv):
        grad_context = mm(TO_F, grad_attn_low, weights[3]).astype(BF16)
        grads = attend_back(qkv, grad_context, real_rows, score_scale)
        return grads, sum(mm(FROM_F, g, weights[j]) for j, g in enumerate(grads))

    def attention_dw(grads, context):
        parts = [mm(WGRAD, g, normed) for g in grads] + [mm(WGRAD, context, grad_attn_low)]
        return jnp.stack([d.astype(BF16).reshape(-1, LANES, width)[:, :head_dim] for d in parts])

    gqkv_far, gnorm_far = attention_back(w_far, qkv_far)
    dw_far2 = attention_dw(gqkv_far, context_far)
    dw_far_from_sib = sib(dw_far2[:, heads:])
    dw_from_far = across((dw_far2[:, :heads].astype(F32) + dw_far_from_sib.astype(F32)).astype(BF16))
    gqkv_near, gnorm_near = attention_back(w_near, qkv_near)
    grad_normed = (gnorm_near + gnorm_far).astype(BF16)
    grad_x_ln, grad_gain, grad_bias = norm1_pull(grad_normed)
    gh_own = (grad_x_one + grad_x_ln).astype(BF16)
    gh_far = across(gh_own)
    gh_sib = sib(gh_own)
    gh_far_sib = sib(gh_far)
    dw_near2 = attention_dw(gqkv_near, context_near)
    dw_near_from_sib = sib(dw_near2[:, heads:])
    grad_hidden = by_tp(tp, (gh_own, gh_sib, gh_far, gh_far_sib), [
        lambda o, s, f, fs: jnp.concatenate([o, s, f, fs], axis=0),
        lambda o, s, f, fs: jnp.concatenate([s, o, fs, f], axis=0),
        lambda o, s, f, fs: jnp.concatenate([f, fs, o, s], axis=0),
        lambda o, s, f, fs: jnp.concatenate([fs, f, s, o], axis=0)])
    dw_own = dw_near2[:, :heads].astype(F32) + dw_near_from_sib.astype(F32) + dw_from_far.astype(F32)
    grad_w_query = jnp.transpose(dw_own[0], (2, 0, 1))
    grad_w_key = jnp.transpose(dw_own[1], (2, 0, 1))
    grad_w_value = jnp.transpose(dw_own[2], (2, 0, 1))
    grad_w_out = dw_own[3]

    mlp_out_late, _ = lax.optimization_barrier((mlp_out, grad_normed))
    grad_gate_mlp = jnp.sum(gx_own_wide * mlp_out_late) * (1.0 - gate_mlp * gate_mlp)
    grad_gate_attn = jnp.sum(grad_x_one * attn_out) * (1.0 - gate_attn * gate_attn)
    small = jnp.concatenate([
        grad_gain, grad_bias, grad_gain_two, grad_bias_two,
        jnp.sum(gate_mlp * gx_own_wide, axis=(0, 1)),
        jnp.sum(own(proj_grad), axis=(0, 1), dtype=F32),
        grad_gate_attn[None], grad_gate_mlp[None]])
    small = small + sib(small)
    small = small + across(small)
    grad_ln = small[:4 * width].reshape(4, width)
    grad_b_fc2 = small[4 * width:5 * width]
    grad_b_proj = small[5 * width:5 * width + proj_dim]
    grad_gates = small[5 * width + proj_dim:]
    return (proj_out, grad_hidden, grad_inter, grad_w_query, grad_w_key, grad_w_value, grad_w_out, grad_ln, grad_gates, grad_w_fc1, grad_b_fc1, grad_w_fc2, grad_b_fc2, grad_w_proj, grad_b_proj)


def solution(mesh):
    tiles_spec = P('dp', None, None)
    inter_spec = P('dp', None, None, None)
    head_cols = P(None, 'tp', None)
    in_specs = (tiles_spec, inter_spec, tiles_spec, head_cols, head_cols, head_cols, P('tp', None, None), P(None, None), P(None), P(None, 'tp'), P('tp'), P('tp', None), P(None), P('tp', None), P(None))
    grad_heads = P('dp', 'tp', None)
    out_specs = (P(('dp', 'tp'), None, None), tiles_spec, inter_spec, grad_heads, grad_heads, grad_heads, P(('dp', 'tp'), None, None), P('dp', None), P('dp'), P('dp', 'tp'), P(('dp', 'tp')), P(('dp', 'tp'), None), P('dp'), P(('dp', 'tp'), None), P('dp'))
    return jax.shard_map(whole_step, mesh=mesh, in_specs=in_specs, out_specs=out_specs, check_vma=False)
```

```python
import functools

import jax
import jax.numpy as jnp
from jax import lax
from jax.experimental import pallas as pl
from jax.experimental.pallas import tpu as pltpu
from jax.sharding import PartitionSpec as P


LN_EPS = 1e-5
TO_F = 'btd,fd->btf'
FROM_F = 'btf,fd->btd'
WGRAD = 'btf,btd->fd'
F32 = jnp.float32
BF16 = jnp.bfloat16
SIB = [(0, 1), (1, 0), (2, 3), (3, 2)]
ACROSS = [(0, 2), (2, 0), (1, 3), (3, 1)]


def layer_norm(values, ln_gain, ln_bias):
    row_mean = jnp.mean(values, axis=-1, keepdims=True)
    centred = values - row_mean
    row_var = jnp.mean(centred * centred, axis=-1, keepdims=True)
    return (centred * lax.rsqrt(row_var + LN_EPS) * ln_gain + ln_bias).astype(BF16)


def mm(eq_form, lhs_in, rhs_in):
    return jnp.einsum(eq_form, lhs_in, rhs_in, preferred_element_type=F32)


LANES = 128


def probs_t(q_block, k_block, real_rows, scale):
    scores = lax.dot_general(k_block, q_block, (((1,), (1,)), ((), ())), preferred_element_type=F32) * scale
    key = lax.broadcasted_iota(jnp.int32, scores.shape, 0)
    scores = jnp.where(key < real_rows, scores, -1e30)
    top = jnp.max(scores, axis=0, keepdims=True)
    expd = jnp.exp(scores - top)
    return expd * (1.0 / jnp.sum(expd, axis=0, keepdims=True))


def attend_kernel(real_rows, scale, count, q_ref, k_ref, v_ref, out_ref):
    for h in range(count):
        cols = pl.ds(h * LANES, LANES)
        probs = probs_t(q_ref[0, :, cols], k_ref[0, :, cols], real_rows, scale).astype(BF16)
        out = lax.dot_general(probs, v_ref[0, :, cols], (((0,), (0,)), ((), ())), preferred_element_type=F32)
        out_ref[0, :, cols] = out.astype(BF16)


def attend_back_kernel(real_rows, scale, count, q_ref, k_ref, v_ref, g_ref, dq_ref, dk_ref, dv_ref):
    for h in range(count):
        cols = pl.ds(h * LANES, LANES)
        q_block, k_block, v_block, g_block = q_ref[0, :, cols], k_ref[0, :, cols], v_ref[0, :, cols], g_ref[0, :, cols]
        probs = probs_t(q_block, k_block, real_rows, scale)
        dv_ref[0, :, cols] = jnp.dot(probs.astype(BF16), g_block, preferred_element_type=F32).astype(BF16)
        dprobs = lax.dot_general(v_block, g_block, (((1,), (1,)), ((), ())), preferred_element_type=F32).astype(BF16).astype(F32)
        dscores = probs * (dprobs - jnp.sum(probs * dprobs, axis=0, keepdims=True))
        dscores = (dscores * scale).astype(BF16)
        dk_ref[0, :, cols] = jnp.dot(dscores, q_block, preferred_element_type=F32).astype(BF16)
        dq = lax.dot_general(dscores, k_block, (((0,), (0,)), ((), ())), preferred_element_type=F32)
        dq_ref[0, :, cols] = dq.astype(BF16)


HEADS_PER_STEP = 4


def attend(q_act, k_act, v_act, real_rows, scale):
    tiles, tokens, cols = q_act.shape
    step = HEADS_PER_STEP * LANES
    spec = pl.BlockSpec((1, tokens, step), lambda t, h: (t, 0, h))
    flops = 4 * tiles * tokens * tokens * cols
    return pl.pallas_call(
        functools.partial(attend_kernel, real_rows, scale, HEADS_PER_STEP),
        out_shape=jax.ShapeDtypeStruct(q_act.shape, BF16),
        grid=(tiles, cols // step),
        in_specs=[spec] * 3,
        out_specs=spec,
        cost_estimate=pl.CostEstimate(flops=4 * flops, bytes_accessed=8 * tiles * tokens * cols, transcendentals=0),
        compiler_params=pltpu.CompilerParams(dimension_semantics=('arbitrary', 'arbitrary')))(q_act, k_act, v_act)


def attend_back(qkv, grad, real_rows, scale):
    tiles, tokens, cols = grad.shape
    step = HEADS_PER_STEP * LANES
    spec = pl.BlockSpec((1, tokens, step), lambda t, h: (t, 0, h))
    shape = jax.ShapeDtypeStruct(grad.shape, BF16)
    flops = 10 * tiles * tokens * tokens * cols
    return pl.pallas_call(
        functools.partial(attend_back_kernel, real_rows, scale, HEADS_PER_STEP),
        out_shape=(shape, shape, shape),
        grid=(tiles, cols // step),
        in_specs=[spec] * 4,
        out_specs=(spec, spec, spec),
        cost_estimate=pl.CostEstimate(flops=4 * flops, bytes_accessed=14 * tiles * tokens * cols, transcendentals=0),
        compiler_params=pltpu.CompilerParams(dimension_semantics=('arbitrary', 'arbitrary')))(*qkv, grad)


def sib(value):
    return lax.ppermute(value, 'tp', SIB)


def across(value):
    return lax.ppermute(value, 'tp', ACROSS)


def gather_piece(quarter):
    quarter = across(quarter)
    return lax.all_gather(quarter, 'dp', axis=0, tiled=True)


def partner_shard(shard, start, count):
    rows = count // 4
    quarter = lax.dynamic_slice_in_dim(shard, start + lax.axis_index('dp') * rows, rows, axis=0)
    return gather_piece(quarter)


def reduce_own(near, far):
    n = near.shape[0] // 2
    from_sib_far = sib(far[n:])
    from_sib_own = sib(near[n:])
    chip_far = (far[:n].astype(F32) + from_sib_far.astype(F32)).astype(BF16)
    from_far = across(chip_far)
    return near[:n].astype(F32) + from_sib_own.astype(F32) + from_far.astype(F32)


def by_tp(tp, parts, builders):
    return lax.switch(tp, [lambda *p, b=b: b(*p) for b in builders], *parts)


def unfilled(shape, dtype):
    return pl.pallas_call(
        lambda out_ref: None,
        out_shape=jax.ShapeDtypeStruct(shape, dtype),
        out_specs=pl.BlockSpec(memory_space=pl.ANY),
        name='unfilled')()


def put_rows(buffer, piece, start):
    return lax.dynamic_update_slice_in_dim(buffer, piece, start, axis=0)


def whole_step(hidden, inter_feats, proj_grad, w_query, w_key, w_value, w_out, ln_params, gate_params, w_fc1, b_fc1, w_fc2, b_fc2, w_proj, b_proj):
    tiles, tokens, width = hidden.shape
    real_rows, proj_dim = proj_grad.shape[1:]
    ninter = inter_feats.shape[2]
    own_n = tiles // 4
    tp = lax.axis_index('tp')
    core = tp & 1
    first = tp * own_n
    inter_t = jnp.transpose(inter_feats, (0, 2, 1, 3))
    row_ok = (jnp.arange(tokens) < real_rows)[None, :, None]
    gate_attn = jnp.tanh(gate_params[0])
    gate_mlp = jnp.tanh(gate_params[1])

    def own(value):
        return lax.dynamic_slice_in_dim(value, first, own_n, axis=0)

    def group_of(value, other):
        return lax.dynamic_slice_in_dim(value, (tp ^ other) * own_n, own_n, axis=0)

    att_own = jnp.stack([jnp.transpose(w_query, (1, 2, 0)), jnp.transpose(w_key, (1, 2, 0)), jnp.transpose(w_value, (1, 2, 0)), w_out])
    heads, head_dim = att_own.shape[1:3]
    att_rows = att_own.reshape(4 * heads * head_dim, width)
    att_sib = sib(att_rows)
    att_far = partner_shard(att_rows, 0, att_rows.shape[0])
    att_far_sib = sib(att_far)

    score_scale = head_dim ** -0.5

    def head_group(*shards):
        group = jnp.concatenate([v.reshape(4, heads, head_dim, width) for v in shards], axis=1)
        group = jnp.pad(group, ((0, 0), (0, 0), (0, LANES - head_dim), (0, 0)))
        return group.reshape(4, -1, width)

    shard_rows = w_proj.shape[0]
    half = shard_rows - width
    wp_sib = sib(w_proj)

    def far_head(own_core):
        quarter = half // 4
        start = core * half + lax.axis_index('dp') * quarter
        piece = jnp.where(core == own_core, lax.dynamic_slice_in_dim(w_proj, start, quarter), lax.dynamic_slice_in_dim(wp_sib, start, quarter))
        mine = gather_piece(piece)
        return mine, sib(mine)

    even, even_sib = far_head(0)
    odd, odd_sib = far_head(1)
    tail = partner_shard(w_proj, width, half)
    tail_sib = sib(tail)
    far_even = 2 * (1 - tp // 2) * shard_rows
    far_odd = far_even + shard_rows
    wp_all = unfilled((4 * shard_rows, proj_dim), BF16)
    wp_all = put_rows(wp_all, w_proj, tp * shard_rows)
    wp_all = put_rows(wp_all, wp_sib, (tp ^ 1) * shard_rows)
    wp_all = put_rows(wp_all, even, far_even + core * half)
    wp_all = put_rows(wp_all, even_sib, far_even + (1 - core) * half)
    wp_all = put_rows(wp_all, odd, far_odd + core * half)
    wp_all = put_rows(wp_all, odd_sib, far_odd + (1 - core) * half)
    wp_all = put_rows(wp_all, tail, (tp ^ 2) * shard_rows + width)
    wp_all = put_rows(wp_all, tail_sib, (tp ^ 3) * shard_rows + width)
    wp_planes = wp_all.reshape(ninter + 1, width, proj_dim)
    wp_first = by_tp(tp, (w_proj, wp_sib, even, even_sib), [
        lambda o, s, e, es: o[:width],
        lambda o, s, e, es: s[:width],
        lambda o, s, e, es: jnp.concatenate([e, es], axis=0),
        lambda o, s, e, es: jnp.concatenate([es, e], axis=0)])

    pg = jnp.pad(proj_grad, ((0, 0), (0, tokens - real_rows), (0, 0)))

    hid_own = own(hidden).astype(F32)
    normed, norm1_pull = jax.vjp(layer_norm, hid_own, ln_params[0], ln_params[1])

    def attention(weights):
        qkv = [mm(TO_F, normed, weights[j]).astype(BF16) for j in range(3)]
        context = attend(*qkv, real_rows, score_scale)
        return mm(FROM_F, context, weights[3]), context, qkv

    w_near = head_group(att_rows, att_sib)
    attn_near, context_near, qkv_near = attention(w_near)
    w_far = head_group(att_far, att_far_sib)
    attn_far, context_far, qkv_far = attention(w_far)
    attn_out = attn_near + attn_far
    x_one = (hid_own + gate_attn * attn_out).astype(BF16)

    x_one_wide = x_one.astype(F32)
    normed_own, norm2_pull = jax.vjp(layer_norm, x_one_wide, ln_params[2], ln_params[3])
    n2_far = across(normed_own)
    n2_sib = sib(normed_own)
    n2_far_sib = sib(n2_far)
    normed_two = jnp.concatenate([normed_own, n2_sib, n2_far, n2_far_sib], axis=0)

    grad_x_two = mm(TO_F, pg, wp_first).astype(BF16)
    grad_mlp_low = (gate_mlp * grad_x_two.astype(F32)).astype(BF16)
    gx_own = own(grad_x_two)
    gm_all = jnp.concatenate([own(grad_mlp_low), group_of(grad_mlp_low, 1), group_of(grad_mlp_low, 2), group_of(grad_mlp_low, 3)], axis=0)

    grad_act = mm(TO_F, gm_all, w_fc2).astype(BF16)
    pre_act = mm('btd,df->btf', normed_two, w_fc1) + b_fc1
    cdf = 0.5 * (1.0 + lax.erf(pre_act * (0.5 ** 0.5)))
    pdf = jnp.exp(-0.5 * pre_act * pre_act) * 0.3989422804014327
    mlp_act = (pre_act * cdf).astype(BF16)
    grad_pre = grad_act.astype(F32) * (cdf + pre_act * pdf)
    grad_b_fc1 = jnp.sum(grad_pre, axis=(0, 1))
    grad_pre_low = grad_pre.astype(BF16)
    pair = 2 * own_n
    gn_far = mm(TO_F, grad_pre_low[pair:], w_fc1).astype(BF16)
    gn_near = mm(TO_F, grad_pre_low[:pair], w_fc1).astype(BF16)
    mlp_sum = mm(FROM_F, mlp_act, w_fc2).astype(BF16)
    grad_normed_two = reduce_own(gn_near, gn_far).astype(BF16)
    mlp_out = reduce_own(mlp_sum[:pair], mlp_sum[pair:]) + b_fc2
    grad_w_fc1 = mm(WGRAD, normed_two, grad_pre_low)
    grad_w_fc2 = mm(WGRAD, mlp_act, gm_all)

    x_two = jnp.where(row_ok, (x_one_wide + gate_mlp * mlp_out).astype(BF16), 0)
    feats_own = jnp.concatenate([x_two[:, None, :real_rows], own(inter_t)[:, :, :real_rows]], axis=1)
    proj_own = mm('bntc,ncp->btp', feats_own, wp_planes)
    proj_out = (proj_own + b_proj).astype(BF16)
    x_two_far = lax.ppermute(x_two, 'tp', [(2, 0), (3, 1)])
    x_two_sib = lax.ppermute(x_two, 'tp', [(1, 0)])
    x_two_far_sib = lax.ppermute(x_two_far, 'tp', [(1, 0)])
    part = by_tp(tp, (inter_t,), [
        lambda i: i[:, 0, :, :half],
        lambda i: i[:, 0, :, half:],
        lambda i: i[:, 3, :, :half],
        lambda i: i[:, 3, :, half:]])
    grad_w_proj = unfilled((shard_rows, proj_dim), F32)
    grad_w_proj = put_rows(grad_w_proj, mm(WGRAD, part, pg), (1 - core) * width)
    plane = by_tp(tp, (inter_t, x_two, x_two_sib, x_two_far, x_two_far_sib), [
        lambda i, o, s, f, fs: jnp.concatenate([o, s, f, fs], axis=0),
        lambda i, o, s, f, fs: i[:, 1],
        lambda i, o, s, f, fs: i[:, 2],
        lambda i, o, s, f, fs: i[:, 4]])
    grad_w_proj = put_rows(grad_w_proj, mm(WGRAD, plane, pg), core * half)

    half_tiles = tiles // 2
    grad_inter = unfilled((tiles, ninter, tokens, width), BF16)
    gi_sib = []
    for n in range(ninter):
        pg_half = lax.dynamic_slice_in_dim(pg, core * half_tiles, half_tiles, axis=0)
        gi_half = mm(TO_F, pg_half, wp_planes[n + 1]).astype(BF16)
        grad_inter = lax.dynamic_update_slice(grad_inter, gi_half[:, None], (core * half_tiles, n, 0, 0))
        gi_sib.append(sib(gi_half))
    for n in range(ninter):
        grad_inter = lax.dynamic_update_slice(grad_inter, gi_sib[n][:, None], ((1 - core) * half_tiles, n, 0, 0))
    grad_inter = jnp.transpose(grad_inter, (0, 2, 1, 3))

    grad_x_ln_two, grad_gain_two, grad_bias_two = norm2_pull(grad_normed_two)
    gx_own_wide = gx_own.astype(F32)
    grad_x_one = (gx_own_wide + grad_x_ln_two).astype(BF16).astype(F32)
    grad_attn_low = (gate_attn * grad_x_one).astype(BF16)

    def attention_back(weights, qkv):
        grad_context = mm(TO_F, grad_attn_low, weights[3]).astype(BF16)
        grads = attend_back(qkv, grad_context, real_rows, score_scale)
        return grads, sum(mm(FROM_F, g, weights[j]) for j, g in enumerate(grads))

    def attention_dw(grads, context):
        parts = [mm(WGRAD, g, normed) for g in grads] + [mm(WGRAD, context, grad_attn_low)]
        return jnp.stack([d.astype(BF16).reshape(-1, LANES, width)[:, :head_dim] for d in parts])

    gqkv_far, gnorm_far = attention_back(w_far, qkv_far)
    dw_far2 = attention_dw(gqkv_far, context_far)
    dw_far_from_sib = sib(dw_far2[:, heads:])
    dw_from_far = across((dw_far2[:, :heads].astype(F32) + dw_far_from_sib.astype(F32)).astype(BF16))
    gqkv_near, gnorm_near = attention_back(w_near, qkv_near)
    grad_normed = (gnorm_near + gnorm_far).astype(BF16)
    grad_x_ln, grad_gain, grad_bias = norm1_pull(grad_normed)
    gh_own = (grad_x_one + grad_x_ln).astype(BF16)
    gh_far = across(gh_own)
    gh_sib = sib(gh_own)
    gh_far_sib = sib(gh_far)
    dw_near2 = attention_dw(gqkv_near, context_near)
    dw_near_from_sib = sib(dw_near2[:, heads:])
    grad_hidden = by_tp(tp, (gh_own, gh_sib, gh_far, gh_far_sib), [
        lambda o, s, f, fs: jnp.concatenate([o, s, f, fs], axis=0),
        lambda o, s, f, fs: jnp.concatenate([s, o, fs, f], axis=0),
        lambda o, s, f, fs: jnp.concatenate([f, fs, o, s], axis=0),
        lambda o, s, f, fs: jnp.concatenate([fs, f, s, o], axis=0)])
    dw_own = dw_near2[:, :heads].astype(F32) + dw_near_from_sib.astype(F32) + dw_from_far.astype(F32)
    grad_w_query = jnp.transpose(dw_own[0], (2, 0, 1))
    grad_w_key = jnp.transpose(dw_own[1], (2, 0, 1))
    grad_w_value = jnp.transpose(dw_own[2], (2, 0, 1))
    grad_w_out = dw_own[3]

    mlp_out_late, _ = lax.optimization_barrier((mlp_out, grad_normed))
    grad_gate_mlp = jnp.sum(gx_own_wide * mlp_out_late) * (1.0 - gate_mlp * gate_mlp)
    grad_gate_attn = jnp.sum(grad_x_one * attn_out) * (1.0 - gate_attn * gate_attn)
    small = jnp.concatenate([
        grad_gain, grad_bias, grad_gain_two, grad_bias_two,
        jnp.sum(gate_mlp * gx_own_wide, axis=(0, 1)),
        jnp.sum(own(proj_grad), axis=(0, 1), dtype=F32),
        grad_gate_attn[None], grad_gate_mlp[None]])
    small = small + sib(small)
    small = small + across(small)
    grad_ln = small[:4 * width].reshape(4, width)
    grad_b_fc2 = small[4 * width:5 * width]
    grad_b_proj = small[5 * width:5 * width + proj_dim]
    grad_gates = small[5 * width + proj_dim:]
    return (proj_out, grad_hidden, grad_inter, grad_w_query, grad_w_key, grad_w_value, grad_w_out, grad_ln, grad_gates, grad_w_fc1, grad_b_fc1, grad_w_fc2, grad_b_fc2, grad_w_proj, grad_b_proj)


def solution(mesh):
    tiles_spec = P('dp', None, None)
    inter_spec = P('dp', None, None, None)
    head_cols = P(None, 'tp', None)
    in_specs = (tiles_spec, inter_spec, tiles_spec, head_cols, head_cols, head_cols, P('tp', None, None), P(None, None), P(None), P(None, 'tp'), P('tp'), P('tp', None), P(None), P('tp', None), P(None))
    grad_heads = P('dp', 'tp', None)
    out_specs = (P(('dp', 'tp'), None, None), tiles_spec, inter_spec, grad_heads, grad_heads, grad_heads, P(('dp', 'tp'), None, None), P('dp', None), P('dp'), P('dp', 'tp'), P(('dp', 'tp')), P(('dp', 'tp'), None), P('dp'), P(('dp', 'tp'), None), P('dp'))
    return jax.shard_map(whole_step, mesh=mesh, in_specs=in_specs, out_specs=out_specs, check_vma=False)
```
